256 devices in a mesh: tp: 16 (over z, core), dp: 16 (over x, y).
Axes of the slice: x: 4, y: 4, z: 8, core: 2. Of those that a mesh axis runs over, the one named last changes fastest.
Arguments:
- partials: bfloat16 [16, 512, 16384], P('tp', 'dp'), parts along dimension 1, may hold values from -1.5 to 1.5
- residual: bfloat16 [512, 16384], P('dp'), parts along dimension 0, may hold values from -150 to 150
- gain: bfloat16 [16384], replicated, may hold values from 0.25 to 1.75
- queries: bfloat16 [512, 16384], P('dp', 'tp'), parts along dimension 0, may hold values from -4000 to 4000
- key_cache: bfloat16 [16, 512, 512, 128], P('tp', 'dp'), parts along dimension 1, may hold values from -6 to 6, as said below
- value_cache: bfloat16 [16, 512, 512, 128], P('tp', 'dp'), parts along dimension 1, may hold values from -6 to 6, as said below
- lengths: int32 [512], P('dp'), parts along dimension 0, may hold values from 64 to 512
Outputs:
- new_residual: bfloat16 [512, 16384], P('dp'), parts along dimension 0
- normed: bfloat16 [512, 16384], P('dp'), parts along dimension 0
- token_peak: float32 [512], P('dp'), parts along dimension 0
- attended: bfloat16 [512, 16384], P('dp', 'tp'), parts along dimension 0
The draws below stay inside these ranges and needn't reach their ends.
There are 16 independent parts, one for each index of `dp`. The reference program is written for one: setup_inputs(seed, part) draws one part's arguments, and reference() takes and returns one part's arrays. A program takes and returns all parts, laid end to end along the dimension named above; an argument that names none is the same for every part. Nothing has to cross between parts.
Inputs may be any that keep to these rules, and one draw needn't show every extreme that they name: Slots s and s' of key_cache hold equal keys when s * 8 // 16 == s' * 8 // 16. Slots of value_cache are equal under the same rule as key_cache.
All inputs are finite; a program needn't handle non-finite values.
Results may differ from the reference program's by a relative error of at most 0.0095.
Values may be sent and summed in bfloat16 or wider, within the bound.
No kernel may reach another device: no remote copies, remote signals or barrier semaphores. Data moves between devices by JAX's collectives and lax.ppermute only.
A program may use at most 64 MiB of HBM per device.

```python
import math
import jax
import jax.numpy as jnp
from jax import lax

D = 16384
HEADS = 128
KV_HEADS = 8
HEAD_DIM = 128
TOK_FFN = 32
SEQS = 32
CONTEXT = 512
KV_SLOTS = 16
TERMS = 16


def cache_keys(key):
    base = jnp.clip(jax.random.normal(jax.random.fold_in(key, 101), (KV_HEADS, SEQS, CONTEXT, HEAD_DIM), jnp.float32), -6.0, 6.0)
    keys = base
    return keys


def draw_key_cache(key, part):
    keys = cache_keys(key)
    return jnp.repeat(keys, KV_SLOTS // KV_HEADS, axis=0).astype(jnp.bfloat16)


def draw_value_cache(key, part):
    values = jnp.clip(jax.random.normal(jax.random.fold_in(key, 111), (KV_HEADS, SEQS, CONTEXT, HEAD_DIM), jnp.float32), -6.0, 6.0)
    return jnp.repeat(values, KV_SLOTS // KV_HEADS, axis=0).astype(jnp.bfloat16)


def draw_queries(key, part):
    drawn = jnp.clip(jax.random.normal(jax.random.fold_in(key, 104), (SEQS, HEADS, HEAD_DIM), jnp.float32), -6.0, 6.0)
    return drawn.reshape(SEQS, HEADS * HEAD_DIM).astype(jnp.bfloat16)


def draw_residual(key, part):
    noise = jnp.clip(jax.random.normal(jax.random.fold_in(key, 201), (TOK_FFN, D), jnp.float32), -5.0, 5.0)
    rows = jnp.exp(jax.random.uniform(jax.random.fold_in(key, 202), (TOK_FFN, 1), jnp.float32, 0.0, math.log(10.0)))
    ramp = jnp.exp(jnp.arange(D, dtype=jnp.float32) * (math.log(3.0) / D))[None, :]
    cols = jnp.exp(jax.random.uniform(jax.random.fold_in(key, 203), (1, D), jnp.float32, 0.0, math.log(10.0))) * ramp
    return (noise * rows * cols * 0.1).astype(jnp.bfloat16)


def plant(drawn, own_key, smallest, top_value):
    place = [jax.random.randint(jax.random.fold_in(own_key, axis), (), 0, length) for axis, length in enumerate(drawn.shape)]
    widest = drawn.shape.index(max(drawn.shape))
    next_to = place[:widest] + [(place[widest] + 1) % drawn.shape[widest]] + place[widest + 1:]
    return drawn.at[tuple(place)].set(smallest).at[tuple(next_to)].set(top_value)


def with_spikes(drawn, rng, source, target, parts, factor):
    def block_of(position):
        return (jnp.arange(drawn.shape[position]) // (drawn.shape[position] // parts)).reshape((-1,) + (1,) * (drawn.ndim - 1 - position))

    near = jax.random.permutation(rng, parts)[block_of(target)]
    far = (block_of(target) + parts // 2) % parts
    return jnp.where((block_of(source) == near) | (block_of(source) == far), factor * drawn, drawn)


def shard_levels(stream_key, shape, split, low, largest):
    loudness = 1.0
    for axis_at, blocks in split:
        heights = jax.random.uniform(jax.random.fold_in(jax.random.fold_in(stream_key, 6), axis_at), (blocks,), jnp.float32, low / len(split), largest / len(split))
        loudness = loudness * jnp.repeat(jnp.exp(heights), shape[axis_at] // blocks).reshape((-1,) + (1,) * (len(shape) - 1 - axis_at))
    return loudness


def bell_draw_with(key, shape, spread, limit, pieces, heavy, kind=jnp.bfloat16):
    result = spread * jax.random.normal(key, shape, jnp.float32)
    if pieces:
        result = result * shard_levels(key, shape, pieces, -0.22, 0.18)
    return jnp.clip(with_spikes(result, jax.random.fold_in(key, 3), *heavy), -limit, limit).astype(kind)


def setup_inputs(seed: int = 0, part: int = 0) -> dict:
    seeds = jax.random.split(jax.random.key(seed), 8)
    own_keys = jax.random.split(jax.random.fold_in(seeds[7], part), 8)
    partials = bell_draw_with(own_keys[0], (TERMS, TOK_FFN, D), 0.25, 1.5, ((0, 16),), (0, 2, 16, 2.0))
    residual = draw_residual(jax.random.fold_in(jax.random.fold_in(seeds[7], part), 71), part)
    gain = jnp.clip(1.0 + 0.15 * jax.random.normal(seeds[2], (D,), jnp.float32), 0.25, 1.75).astype(jnp.bfloat16)
    queries = draw_queries(jax.random.fold_in(jax.random.fold_in(seeds[7], part), 71), part)
    key_cache = draw_key_cache(jax.random.fold_in(jax.random.fold_in(seeds[7], part), 71), part)
    value_cache = draw_value_cache(jax.random.fold_in(jax.random.fold_in(seeds[7], part), 71), part)
    lengths = plant(jax.random.randint(own_keys[6], (SEQS,), CONTEXT // 8, CONTEXT + 1), jax.random.fold_in(own_keys[6], 1), CONTEXT // 8, CONTEXT).astype(jnp.int32)
    return dict(partials=partials, residual=residual, gain=gain, queries=queries, key_cache=key_cache, value_cache=value_cache, lengths=lengths)


def reference(partials, residual, gain, queries, key_cache, value_cache, lengths):
    total = lax.optimization_barrier(jnp.sum(partials.astype(jnp.float32), axis=0))
    hsum = residual.astype(jnp.float32) + total
    new_residual = hsum.astype(jnp.bfloat16)
    inv_rms = jax.lax.rsqrt(lax.optimization_barrier(jnp.mean(hsum * hsum, axis=1, keepdims=True)) + 1e-05)
    scaled = hsum * inv_rms * gain.astype(jnp.float32)[None, :]
    normed = scaled.astype(jnp.bfloat16)
    token_peak = lax.optimization_barrier(jnp.max(jnp.abs(scaled), axis=1))
    slots = key_cache.shape[0]
    group = HEADS // slots
    query_f = queries.astype(jnp.float32).reshape(SEQS, slots, group, HEAD_DIM)
    scores = jnp.einsum('bsgd,sbld->bsgl', query_f, key_cache.astype(jnp.float32)) * (1.0 / math.sqrt(HEAD_DIM))
    live = jnp.arange(CONTEXT, dtype=jnp.int32)[None, :] < lengths[:, None]
    scores = jnp.where(live[:, None, None, :], scores, -1e+30)
    top = lax.optimization_barrier(jnp.max(scores, axis=3, keepdims=True))
    expo = jnp.exp(scores - top)
    probs = (expo / lax.optimization_barrier(jnp.sum(expo, axis=3, keepdims=True))).astype(jnp.bfloat16)
    attended = jnp.einsum('bsgl,sbld->bsgd', probs.astype(jnp.float32), value_cache.astype(jnp.float32))
    attended = attended.astype(jnp.bfloat16).reshape(SEQS, HEADS * HEAD_DIM)
    return (new_residual, normed, token_peak, attended)
```

```python
import functools
import math

import jax
import jax.numpy as jnp
from jax import lax
from jax.experimental import pallas as pl
from jax.experimental.pallas import tpu as pltpu
from jax.sharding import PartitionSpec as P


HEAD_DIM = 128
CHIPS = 8
CHUNK = 2048
HALF = 1024
SEQ_GROUPS = 2

f32, bf16 = jnp.float32, jnp.bfloat16
ANY = pl.BlockSpec(memory_space=pl.ANY)
VMEM = pl.BlockSpec(memory_space=pltpu.VMEM)
SMALL = pltpu.CompilerParams(vmem_limit_bytes=16 << 20)


def near(x):
    return pltpu.with_memory_space_constraint(x, pltpu.VMEM)


def far(x):
    return pltpu.with_memory_space_constraint(x, pltpu.HBM)


def onchip(shape, dtype):
    return pltpu.VMEM(shape, dtype)


def place():
    me = lax.axis_index("tp")
    core = lax.rem(me, 2)
    return me // 2, core, 1 - 2 * core


def chunk_at(chip, steps):
    return lax.rem(chip + steps + 2 * CHIPS, CHIPS)


def columns(start, size):
    return pl.ds(pl.multiple_of(start, HALF), size)


def cost(flops, nbytes):
    return pl.CostEstimate(flops=flops, bytes_accessed=nbytes, transcendentals=0)


def along(x, hops):
    pairs = []
    for chip in range(CHIPS):
        pairs.append((2 * chip, 2 * ((chip + hops) % CHIPS)))
        pairs.append((2 * chip + 1, 2 * ((chip - hops) % CHIPS) + 1))
    return lax.ppermute(x, "tp", pairs)


def across(x):
    return lax.ppermute(x, "tp", [(i, i ^ 1) for i in range(2 * CHIPS)])


def handled(chip, core, way):
    return [
        (chunk_at(chip, 4) * CHUNK + core * HALF, HALF),
        (chunk_at(chip, 3 * way) * CHUNK, CHUNK),
        (chunk_at(chip, way) * CHUNK, CHUNK),
        (chunk_at(chip, 2 * way) * CHUNK, CHUNK),
        (chip * CHUNK + core * HALF, HALF),
    ]


def copy_ranges(src, dst, ranges, sems):
    copies, at = [], 0
    for i, (start, size) in enumerate(ranges):
        copies.append(
            pltpu.make_async_copy(
                src.at[:, columns(start, size)], dst.at[:, pl.ds(at, size)], sems.at[i]
            )
        )
        at += size
    return copies


def pack_kernel(p_ref, send_ref, sems):
    chip, core, way = place()
    copies = copy_ranges(p_ref, send_ref, handled(chip, 1 - core, -way), sems)
    for c in copies:
        c.start()
    for c in copies:
        c.wait()


def keep_kernel(p_ref, r_ref, keep_ref, res_ref, sems):
    chip, core, way = place()
    copies = copy_ranges(p_ref, keep_ref, handled(chip, core, way), sems)
    copies.append(
        pltpu.make_async_copy(r_ref.at[:, columns(chip * CHUNK, CHUNK)], res_ref, sems.at[5])
    )
    for c in copies:
        c.start()
    for c in copies:
        c.wait()


def presum_kernel(keep_ref, got_ref, a4_ref, a3_ref, a1_ref, s2_ref, s0_ref):
    at = 0
    for out in (a4_ref, a3_ref, a1_ref, s2_ref, s0_ref):
        size = out.shape[1]
        mine = keep_ref[:, at : at + size].astype(f32)
        out[...] = (mine + got_ref[:, at : at + size].astype(f32)).astype(bf16)
        at += size


def relay_kernel(s2_ref, r3_ref, r4_ref, m_ref):
    _, core, _ = place()
    for half in range(2):
        cols = slice(half * HALF, (half + 1) * HALF)
        both = s2_ref[:, cols].astype(f32) + r3_ref[:, cols].astype(f32)
        here = jnp.where(core == half, 1.0, 0.0).astype(f32)
        m_ref[:, cols] = (both + here * r4_ref[...].astype(f32)).astype(bf16)


def arrive_kernel(r1_ref, rm_ref, s0_ref, t_ref):
    _, core, _ = place()
    for half in range(2):
        cols = slice(half * HALF, (half + 1) * HALF)
        both = r1_ref[:, cols].astype(f32) + rm_ref[:, cols].astype(f32)
        here = jnp.where(core == half, 1.0, 0.0).astype(f32)
        t_ref[:, cols] = (both + here * s0_ref[...].astype(f32)).astype(bf16)


def hsum_kernel(t_ref, rt_ref, res_ref, n_ref):
    total = t_ref[...].astype(f32) + rt_ref[...].astype(f32)
    n_ref[...] = (res_ref[...].astype(f32) + total).astype(bf16)


def fork_kernel(g1_ref, g2_ref, half_ref, both_ref):
    _, core, _ = place()
    half_ref[...] = g2_ref[:, columns(core * HALF, HALF)]
    both_ref[:, :CHUNK] = g1_ref[...]
    both_ref[:, CHUNK:] = g2_ref[...]


def pieces(chip, core, way, n, g1, g2, w12, g3=None, g4=None, w34=None):
    across_ring = chunk_at(chip, 4) * 2
    early = [
        (n, 0, 2 * chip, 2),
        (g1, 0, 2 * chunk_at(chip, -way), 2),
        (g2, 0, 2 * chunk_at(chip, -2 * way), 2),
        (w12, 0, 2 * chunk_at(chip, way), 2),
        (w12, CHUNK, 2 * chunk_at(chip, 2 * way), 2),
    ]
    late = [
        (g3, 0, 2 * chunk_at(chip, -3 * way), 2),
        (g4, 0, across_ring + core, 1),
        (w34, 0, 2 * chunk_at(chip, 3 * way), 2),
        (w34, CHUNK, across_ring + 1 - core, 1),
    ]
    return early, late


def by_half(wide):
    return [(ref, at + k * HALF, block + k) for ref, at, block, n in wide for k in range(n)]


def write_out(wide, out, sems):
    copies = []
    for i, (ref, at, block, n) in enumerate(wide):
        copies.append(
            pltpu.make_async_copy(
                ref.at[:, pl.ds(at, n * HALF)], out.at[:, columns(block * HALF, n * HALF)], sems.at[i]
            )
        )
        copies[-1].start()
    return copies


def add_squares(wide, sq_ref):
    for ref, at, block in by_half(wide):
        part = jnp.zeros(sq_ref.shape[1:], f32)
        for j in range(0, HALF, 128):
            x = ref[:, at + j : at + j + 128].astype(f32)
            part += x * x
        sq_ref[block] = part


def early_kernel(n_ref, g1_ref, g2_ref, w12_ref, res_out, sq_ref, sems):
    early, _ = pieces(*place(), n_ref, g1_ref, g2_ref, w12_ref)
    copies = write_out(early, res_out, sems)
    sq_ref[...] = jnp.zeros_like(sq_ref)
    add_squares(early, sq_ref)
    for copy in copies:
        copy.wait()


def finish_kernel(
    n_ref, g1_ref, g2_ref, w12_ref, g3_ref, g4_ref, w34_ref, gain_ref, early_sq, _,
    res_out, norm_out, peak_ref, y_ref, sq_ref, res_sems, norm_sems,
):
    early, late = pieces(
        *place(), n_ref, g1_ref, g2_ref, w12_ref, g3_ref, g4_ref, w34_ref
    )
    tokens, features = res_out.shape
    copies = write_out(late, res_out, res_sems)
    sq_ref[...] = early_sq[...]
    add_squares(late, sq_ref)
    total = sq_ref[0]
    for block in range(1, features // HALF):
        total += sq_ref[block]
    mean = jnp.sum(total, axis=1, keepdims=True) * (1.0 / features)
    inv = jnp.broadcast_to(lax.rsqrt(mean + 1e-05), (tokens, 128))
    peak = jnp.zeros((tokens, 128), f32)
    for i, (ref, at, block) in enumerate(by_half(early + late)):
        gains = gain_ref[block]
        for j in range(0, HALF, 128):
            x = ref[:, at + j : at + j + 128].astype(f32)
            y = x * inv * gains[:, j : j + 128]
            peak = jnp.maximum(peak, jnp.abs(y))
            y_ref[:, i * HALF + j : i * HALF + j + 128] = y.astype(bf16)
        copies.append(
            pltpu.make_async_copy(
                y_ref.at[:, pl.ds(i * HALF, HALF)],
                norm_out.at[:, columns(block * HALF, HALF)],
                norm_sems.at[i],
            )
        )
        copies[-1].start()
    peak_ref[...] = jnp.max(peak.T, axis=0, keepdims=True)
    for copy in copies:
        copy.wait()


def attend_kernel(first, q_ref, k_ref, v_ref, len_ref, *refs):
    o_ref, q_rows, o_rows, stage, values, sem, v_sems = refs[-7:]
    seqs, width = stage.shape
    heads = width // HEAD_DIM
    rows = seqs * heads
    context = k_ref.shape[1]
    mine = slice(first, first + seqs)
    fetched = [
        pltpu.make_async_copy(v_ref.at[first + i], values.at[i], v_sems.at[i]) for i in range(seqs)
    ]
    for copy in fetched:
        copy.start()
    for h in range(heads):
        cols = slice(h * HEAD_DIM, (h + 1) * HEAD_DIM)
        q_rows[pl.ds(h, seqs, stride=heads), :] = q_ref[mine, cols].astype(f32)
    turned = q_rows[...].T
    owner = lax.broadcasted_iota(jnp.int32, (HEAD_DIM, rows), 1) // heads
    scores = jnp.zeros((context, rows), f32)
    for i in range(seqs):
        own = jnp.where(owner == i, turned, 0.0).astype(bf16)
        scores += jnp.dot(k_ref[first + i], own, preferred_element_type=f32)
    lens = len_ref[mine, :]
    spread = lax.broadcasted_iota(jnp.int32, (seqs, rows), 0)
    spread = spread == lax.broadcasted_iota(jnp.int32, (seqs, rows), 1) // heads
    lens = jnp.sum(jnp.where(spread, lens, 0), axis=0, keepdims=True)
    live = lax.broadcasted_iota(jnp.int32, (context, rows), 0) < lens
    scores = jnp.where(live, scores * (1.0 / math.sqrt(HEAD_DIM)), -1e30)
    expo = jnp.exp(scores - jnp.max(scores, axis=0, keepdims=True))
    probs = (expo * (1.0 / jnp.sum(expo, axis=0, keepdims=True))).T
    for i in range(seqs):
        fetched[i].wait()
        o_rows[i * heads : (i + 1) * heads, :] = jnp.dot(
            probs[i * heads : (i + 1) * heads, :].astype(bf16),
            values[i],
            preferred_element_type=f32,
        )
    for h in range(heads):
        stage[:, h * HEAD_DIM : (h + 1) * HEAD_DIM] = o_rows[
            pl.ds(h, seqs, stride=heads), :
        ].astype(bf16)
    copy = pltpu.make_async_copy(stage, o_ref.at[mine, :], sem)
    copy.start()
    copy.wait()


def attend(queries, keys, values, lens):
    seqs, width = queries.shape
    rows = seqs // SEQ_GROUPS * (width // HEAD_DIM)
    nbytes = 4 * keys.size // SEQ_GROUPS
    out = []
    for g in range(SEQ_GROUPS):
        out = [
            pl.pallas_call(
                functools.partial(attend_kernel, g * (seqs // SEQ_GROUPS)),
                out_shape=jax.ShapeDtypeStruct((seqs, width), bf16),
                in_specs=[VMEM, VMEM, ANY, VMEM] + [ANY] * len(out),
                out_specs=ANY,
                scratch_shapes=[
                    pltpu.VMEM((rows, HEAD_DIM), f32),
                    pltpu.VMEM((rows, HEAD_DIM), f32),
                    pltpu.VMEM((seqs // SEQ_GROUPS, width), bf16),
                    pltpu.VMEM((seqs // SEQ_GROUPS, *values.shape[1:]), bf16),
                    pltpu.SemaphoreType.DMA,
                    pltpu.SemaphoreType.DMA((seqs // SEQ_GROUPS,)),
                ],
                input_output_aliases={4: 0} if out else {},
                cost_estimate=cost(200_000_000, nbytes),
                compiler_params=SMALL,
            )(queries, keys, far(values), near(lens), *out)
        ]
    return out[0]


def summed_and_normed(partial, residual, gain):
    tokens, features = partial.shape
    dma = pltpu.SemaphoreType.DMA

    def held(width):
        return onchip((tokens, width), bf16)

    def call(kernel, outs, *args, in_specs=None, scratch=(), flops=1000):
        args = [far(a) if in_specs else near(a) for a in args]
        return pl.pallas_call(
            kernel,
            out_shape=outs,
            in_specs=in_specs or [VMEM] * len(args),
            out_specs=jax.tree.map(lambda _: VMEM, outs),
            scratch_shapes=list(scratch),
            cost_estimate=cost(flops, 1 << 20),
            compiler_params=SMALL,
        )(*args)

    send = call(pack_kernel, held(8192), partial, in_specs=[ANY], scratch=[dma((5,))])
    got = across(send)
    keep, res = call(
        keep_kernel, (held(8192), held(CHUNK)), partial, residual,
        in_specs=[ANY, ANY], scratch=[dma((6,))],
    )
    a4, a3, a1, s2, s0 = call(
        presum_kernel, (held(HALF), held(CHUNK), held(CHUNK), held(CHUNK), held(HALF)), keep, got
    )
    r4 = along(a4, 2)
    r3 = along(a3, 1)
    r1 = along(a1, 1)
    m = call(relay_kernel, held(CHUNK), s2, r3, r4)
    rm = along(m, 2)
    t = call(arrive_kernel, held(CHUNK), r1, rm, s0)
    rt = across(t)
    n = call(hsum_kernel, held(CHUNK), t, rt, res)
    g2 = along(n, 2)
    g1 = along(n, 1)
    half, both = call(fork_kernel, (held(HALF), held(2 * CHUNK)), g1, g2)
    g3 = along(g2, 1)
    g4 = along(half, 2)
    w12 = across(both)
    last = jnp.concatenate([g3, g4], axis=1)
    w34 = across(last)
    blocks = features // HALF
    gains = gain.astype(f32).reshape(blocks, 1, HALF)
    whole = jax.ShapeDtypeStruct((tokens, features), bf16)
    begun, squares = pl.pallas_call(
        early_kernel,
        out_shape=(whole, onchip((blocks, tokens, 128), f32)),
        in_specs=[VMEM] * 4,
        out_specs=(ANY, VMEM),
        scratch_shapes=[dma((5,))],
        cost_estimate=cost(1_000_000, 1 << 20),
        compiler_params=SMALL,
        name="early",
    )(*map(near, (n, g1, g2, w12)))
    res_out, norm_out, peak = pl.pallas_call(
        finish_kernel,
        out_shape=(whole, whole, jax.ShapeDtypeStruct((1, tokens), f32)),
        in_specs=[VMEM] * 9 + [ANY],
        out_specs=(ANY, ANY, VMEM),
        scratch_shapes=[
            pltpu.VMEM((tokens, features), bf16),
            pltpu.VMEM((blocks, tokens, 128), f32),
            dma((4,)),
            dma((blocks,)),
        ],
        input_output_aliases={9: 0},
        cost_estimate=cost(1_000_000, 4 << 20),
        compiler_params=SMALL,
        name="finish",
    )(*map(near, (n, g1, g2, w12, g3, g4, w34, gains, squares)), begun)
    return res_out, norm_out, peak.reshape(tokens)


def on_device(partials, residual, gain, queries, key_cache, value_cache, lengths):
    lens = jnp.broadcast_to(lengths[:, None], (lengths.shape[0], 128))
    attended = attend(queries, key_cache[0], value_cache[0], lens)
    new_residual, normed, token_peak = summed_and_normed(partials[0], residual, gain)
    return (new_residual, normed, token_peak, attended)


def solution(mesh):
    return jax.shard_map(
        on_device,
        mesh=mesh,
        in_specs=(
            P("tp", "dp", None),
            P("dp", None),
            P(),
            P("dp", "tp"),
            P("tp", "dp", None, None),
            P("tp", "dp", None, None),
            P("dp"),
        ),
        out_specs=(P("dp", None), P("dp", None), P("dp"), P("dp", "tp")),
        check_vma=False,
    )
```

```python
import functools
import math

import jax
import jax.numpy as jnp
from jax import lax
from jax.experimental import pallas as pl
from jax.experimental.pallas import tpu as pltpu
from jax.sharding import PartitionSpec as P


HEAD_DIM = 128
CHIPS = 8
CHUNK = 2048
HALF = 1024
SEQ_GROUPS = 2

f32, bf16 = jnp.float32, jnp.bfloat16
ANY = pl.BlockSpec(memory_space=pl.ANY)
VMEM = pl.BlockSpec(memory_space=pltpu.VMEM)
SMALL = pltpu.CompilerParams(vmem_limit_bytes=16 << 20)


def near(x):
    return pltpu.with_memory_space_constraint(x, pltpu.VMEM)


def far(x):
    return pltpu.with_memory_space_constraint(x, pltpu.HBM)


def onchip(shape, dtype):
    return pltpu.VMEM(shape, dtype)


def place():
    me = lax.axis_index("tp")
    core = lax.rem(me, 2)
    return me // 2, core, 1 - 2 * core


def chunk_at(chip, steps):
    return lax.rem(chip + steps + 2 * CHIPS, CHIPS)


def columns(start, size):
    return pl.ds(pl.multiple_of(start, HALF), size)


def cost(flops, nbytes):
    return pl.CostEstimate(flops=flops, bytes_accessed=nbytes, transcendentals=0)


def along(x, hops):
    pairs = []
    for chip in range(CHIPS):
        pairs.append((2 * chip, 2 * ((chip + hops) % CHIPS)))
        pairs.append((2 * chip + 1, 2 * ((chip - hops) % CHIPS) + 1))
    return lax.ppermute(x, "tp", pairs)


def across(x):
    return lax.ppermute(x, "tp", [(i, i ^ 1) for i in range(2 * CHIPS)])


def handled(chip, core, way):
    return [
        (chunk_at(chip, 3 * way) * CHUNK, CHUNK),
        (chunk_at(chip, way) * CHUNK, CHUNK),
        (chunk_at(chip, 2 * way) * CHUNK, CHUNK),
        (chunk_at(chip, 4) * CHUNK + core * HALF, HALF),
        (chip * CHUNK + core * HALF, HALF),
    ]


def copy_ranges(src, dst, ranges, sems):
    copies, at = [], 0
    for i, (start, size) in enumerate(ranges):
        copies.append(
            pltpu.make_async_copy(
                src.at[:, columns(start, size)], dst.at[:, pl.ds(at, size)], sems.at[i]
            )
        )
        at += size
    return copies


def pack_kernel(p_ref, send_ref, sems):
    chip, core, way = place()
    copies = copy_ranges(p_ref, send_ref, handled(chip, 1 - core, -way), sems)
    for c in copies:
        c.start()
    for c in copies:
        c.wait()


def keep_kernel(p_ref, r_ref, keep_ref, res_ref, sems):
    chip, core, way = place()
    copies = copy_ranges(p_ref, keep_ref, handled(chip, core, way), sems)
    copies.append(
        pltpu.make_async_copy(r_ref.at[:, columns(chip * CHUNK, CHUNK)], res_ref, sems.at[5])
    )
    for c in copies:
        c.start()
    for c in copies:
        c.wait()


def presum_kernel(keep_ref, got_ref, *outs):
    at = 0
    for out in outs:
        size = out.shape[1]
        mine = keep_ref[:, at : at + size].astype(f32)
        out[...] = (mine + got_ref[:, at : at + size].astype(f32)).astype(bf16)
        at += size


def relay_kernel(s2_ref, r3_ref, m_ref):
    m_ref[...] = (s2_ref[...].astype(f32) + r3_ref[...].astype(f32)).astype(bf16)


def arrive_kernel(r1_ref, rm_ref, r4_ref, own_ref, t_ref):
    _, core, _ = place()
    extra = r4_ref[...].astype(f32) + own_ref[...].astype(f32)
    for half in range(2):
        cols = slice(half * HALF, (half + 1) * HALF)
        both = r1_ref[:, cols].astype(f32) + rm_ref[:, cols].astype(f32)
        here = jnp.where(core == half, extra, jnp.zeros_like(extra))
        t_ref[:, cols] = (both + here).astype(bf16)


def hsum_kernel(t_ref, rt_ref, res_ref, n_ref, half_ref):
    _, core, _ = place()
    total = t_ref[...].astype(f32) + rt_ref[...].astype(f32)
    n = (res_ref[...].astype(f32) + total).astype(bf16)
    n_ref[...] = n
    half_ref[...] = jnp.where(core == 0, n[:, :HALF], n[:, HALF:])


def pieces(chip, core, way, n, g1, g2, w12, last=None, w34=None):
    opposite = 2 * chunk_at(chip, 4)
    early = [
        (n, 0, 2 * chip, 2),
        (g1, 0, 2 * chunk_at(chip, -way), 2),
        (g2, 0, 2 * chunk_at(chip, -2 * way), 2),
        (w12, 0, 2 * chunk_at(chip, way), 2),
        (w12, CHUNK, 2 * chunk_at(chip, 2 * way), 2),
    ]
    late = [
        (last, 0, 2 * chunk_at(chip, -3 * way), 2),
        (last, CHUNK, opposite + core, 1),
        (w34, 0, 2 * chunk_at(chip, 3 * way), 2),
        (w34, CHUNK, opposite + 1 - core, 1),
    ]
    return early, late


def by_half(wide):
    return [(ref, at + k * HALF, block + k) for ref, at, block, n in wide for k in range(n)]


def write_out(wide, out, sems):
    copies = []
    for i, (ref, at, block, n) in enumerate(wide):
        copies.append(
            pltpu.make_async_copy(
                ref.at[:, pl.ds(at, n * HALF)], out.at[:, columns(block * HALF, n * HALF)], sems.at[i]
            )
        )
        copies[-1].start()
    return copies


def add_squares(wide, sq_ref):
    for ref, at, block in by_half(wide):
        part = jnp.zeros(sq_ref.shape[1:], f32)
        for j in range(0, HALF, 128):
            x = ref[:, at + j : at + j + 128].astype(f32)
            part += x * x
        sq_ref[block] = part


def early_kernel(n_ref, g1_ref, g2_ref, w12_ref, res_out, sq_ref, sems):
    early, _ = pieces(*place(), n_ref, g1_ref, g2_ref, w12_ref)
    copies = write_out(early, res_out, sems)
    sq_ref[...] = jnp.zeros_like(sq_ref)
    add_squares(early, sq_ref)
    for copy in copies:
        copy.wait()


def finish_kernel(
    n_ref, g1_ref, g2_ref, w12_ref, last_ref, w34_ref, gain_ref, early_sq, _,
    res_out, norm_out, peak_ref, y_ref, sq_ref, res_sems, norm_sems,
):
    early, late = pieces(*place(), n_ref, g1_ref, g2_ref, w12_ref, last_ref, w34_ref)
    tokens, features = res_out.shape
    copies = write_out(late, res_out, res_sems)
    sq_ref[...] = early_sq[...]
    add_squares(late, sq_ref)
    total = sq_ref[0]
    for block in range(1, features // HALF):
        total += sq_ref[block]
    mean = jnp.sum(total, axis=1, keepdims=True) * (1.0 / features)
    inv = jnp.broadcast_to(lax.rsqrt(mean + 1e-05), (tokens, 128))
    peak = jnp.zeros((tokens, 128), f32)
    for i, (ref, at, block) in enumerate(by_half(early + late)):
        gains = gain_ref[block]
        for j in range(0, HALF, 128):
            x = ref[:, at + j : at + j + 128].astype(f32)
            y = x * inv * gains[:, j : j + 128]
            peak = jnp.maximum(peak, jnp.abs(y))
            y_ref[:, i * HALF + j : i * HALF + j + 128] = y.astype(bf16)
        copies.append(
            pltpu.make_async_copy(
                y_ref.at[:, pl.ds(i * HALF, HALF)],
                norm_out.at[:, columns(block * HALF, HALF)],
                norm_sems.at[i],
            )
        )
        copies[-1].start()
    peak_ref[...] = jnp.max(peak.T, axis=0, keepdims=True)
    for copy in copies:
        copy.wait()


def attend_kernel(first, q_ref, k_ref, v_ref, len_ref, *refs):
    o_ref, q_rows, o_rows, stage, values, sem, v_sem = refs[-7:]
    seqs, width = stage.shape
    heads = width // HEAD_DIM
    rows = seqs * heads
    context = k_ref.shape[1]
    mine = slice(first, first + seqs)
    fetched = pltpu.make_async_copy(v_ref.at[mine], values, v_sem)
    fetched.start()
    for h in range(heads):
        cols = slice(h * HEAD_DIM, (h + 1) * HEAD_DIM)
        q_rows[pl.ds(h, seqs, stride=heads), :] = q_ref[mine, cols].astype(f32)
    turned = q_rows[...].T
    owner = lax.broadcasted_iota(jnp.int32, (HEAD_DIM, rows), 1) // heads
    scores = jnp.zeros((context, rows), f32)
    for i in range(seqs):
        own = jnp.where(owner == i, turned, 0.0).astype(bf16)
        scores += jnp.dot(k_ref[first + i], own, preferred_element_type=f32)
    lens = len_ref[mine, :]
    spread = lax.broadcasted_iota(jnp.int32, (seqs, rows), 0)
    spread = spread == lax.broadcasted_iota(jnp.int32, (seqs, rows), 1) // heads
    lens = jnp.sum(jnp.where(spread, lens, 0), axis=0, keepdims=True)
    live = lax.broadcasted_iota(jnp.int32, (context, rows), 0) < lens
    scores = jnp.where(live, scores * (1.0 / math.sqrt(HEAD_DIM)), -1e30)
    expo = jnp.exp(scores - jnp.max(scores, axis=0, keepdims=True))
    probs = (expo * (1.0 / jnp.sum(expo, axis=0, keepdims=True))).T
    fetched.wait()
    for i in range(seqs):
        o_rows[i * heads : (i + 1) * heads, :] = jnp.dot(
            probs[i * heads : (i + 1) * heads, :].astype(bf16),
            values[i],
            preferred_element_type=f32,
        )
    for h in range(heads):
        stage[:, h * HEAD_DIM : (h + 1) * HEAD_DIM] = o_rows[
            pl.ds(h, seqs, stride=heads), :
        ].astype(bf16)
    copy = pltpu.make_async_copy(stage, o_ref.at[mine, :], sem)
    copy.start()
    copy.wait()


def attend(queries, keys, values, lens):
    seqs, width = queries.shape
    rows = seqs // SEQ_GROUPS * (width // HEAD_DIM)
    nbytes = 4 * keys.size // SEQ_GROUPS
    out = []
    for g in range(SEQ_GROUPS):
        out = [
            pl.pallas_call(
                functools.partial(attend_kernel, g * (seqs // SEQ_GROUPS)),
                out_shape=jax.ShapeDtypeStruct((seqs, width), bf16),
                in_specs=[VMEM, VMEM, ANY, VMEM] + [ANY] * len(out),
                out_specs=ANY,
                scratch_shapes=[
                    pltpu.VMEM((rows, HEAD_DIM), f32),
                    pltpu.VMEM((rows, HEAD_DIM), f32),
                    pltpu.VMEM((seqs // SEQ_GROUPS, width), bf16),
                    pltpu.VMEM((seqs // SEQ_GROUPS, *values.shape[1:]), bf16),
                    pltpu.SemaphoreType.DMA,
                    pltpu.SemaphoreType.DMA,
                ],
                input_output_aliases={4: 0} if out else {},
                cost_estimate=cost(200_000_000, nbytes),
                compiler_params=SMALL,
            )(queries, keys, far(values), near(lens), *out)
        ]
    return out[0]


def summed_and_normed(partial, residual, gain):
    tokens, features = partial.shape
    dma = pltpu.SemaphoreType.DMA

    def held(width):
        return onchip((tokens, width), bf16)

    def call(kernel, outs, *args, in_specs=None, scratch=(), flops=1000):
        args = [far(a) if in_specs else near(a) for a in args]
        return pl.pallas_call(
            kernel,
            out_shape=outs,
            in_specs=in_specs or [VMEM] * len(args),
            out_specs=jax.tree.map(lambda _: VMEM, outs),
            scratch_shapes=list(scratch),
            cost_estimate=cost(flops, 1 << 20),
            compiler_params=SMALL,
        )(*args)

    send = call(pack_kernel, held(8192), partial, in_specs=[ANY], scratch=[dma((5,))])
    got = across(send)
    keep, res = call(
        keep_kernel, (held(8192), held(CHUNK)), partial, residual,
        in_specs=[ANY, ANY], scratch=[dma((6,))],
    )
    a3, a1, s2, a4, own = call(
        presum_kernel, (held(CHUNK), held(CHUNK), held(CHUNK), held(HALF), held(HALF)), keep, got
    )
    r3 = along(a3, 1)
    r1 = along(a1, 1)
    r4 = along(a4, 4)
    m = call(relay_kernel, held(CHUNK), s2, r3)
    rm = along(m, 2)
    t = call(arrive_kernel, held(CHUNK), r1, rm, r4, own)
    rt = across(t)
    n, half = call(hsum_kernel, (held(CHUNK), held(HALF)), t, rt, res)
    g2 = along(n, 2)
    g1 = along(n, 1)
    g4 = along(half, 4)
    g3 = along(g2, 1)
    both = jnp.concatenate([g1, g2], axis=1)
    w12 = across(both)
    last = jnp.concatenate([g3, g4], axis=1)
    w34 = across(last)
    blocks = features // HALF
    gains = gain.astype(f32).reshape(blocks, 1, HALF)
    whole = jax.ShapeDtypeStruct((tokens, features), bf16)
    begun, squares = pl.pallas_call(
        early_kernel,
        out_shape=(whole, onchip((blocks, tokens, 128), f32)),
        in_specs=[VMEM] * 4,
        out_specs=(ANY, VMEM),
        scratch_shapes=[dma((5,))],
        cost_estimate=cost(1_000_000, 1 << 20),
        compiler_params=SMALL,
        name="early",
    )(*map(near, (n, g1, g2, w12)))
    res_out, norm_out, peak = pl.pallas_call(
        finish_kernel,
        out_shape=(whole, whole, jax.ShapeDtypeStruct((1, tokens), f32)),
        in_specs=[VMEM] * 8 + [ANY],
        out_specs=(ANY, ANY, VMEM),
        scratch_shapes=[
            pltpu.VMEM((tokens, features), bf16),
            pltpu.VMEM((blocks, tokens, 128), f32),
            dma((4,)),
            dma((blocks,)),
        ],
        input_output_aliases={8: 0},
        cost_estimate=cost(1_000_000, 4 << 20),
        compiler_params=SMALL,
        name="finish",
    )(*map(near, (n, g1, g2, w12, last, w34, gains, squares)), begun)
    return res_out, norm_out, peak.reshape(tokens)


def on_device(partials, residual, gain, queries, key_cache, value_cache, lengths):
    lens = jnp.broadcast_to(lengths[:, None], (lengths.shape[0], 128))
    attended = attend(queries, key_cache[0], value_cache[0], lens)
    new_residual, normed, token_peak = summed_and_normed(partials[0], residual, gain)
    return (new_residual, normed, token_peak, attended)


def solution(mesh):
    return jax.shard_map(
        on_device,
        mesh=mesh,
        in_specs=(
            P("tp", "dp", None),
            P("dp", None),
            P(),
            P("dp", "tp"),
            P("tp", "dp", None, None),
            P("tp", "dp", None, None),
            P("dp"),
        ),
        out_specs=(P("dp", None), P("dp", None), P("dp"), P("dp", "tp")),
        check_vma=False,
    )
```

```python
import functools
import math

import jax
import jax.numpy as jnp
from jax import lax
from jax.experimental import pallas as pl
from jax.experimental.pallas import tpu as pltpu
from jax.sharding import PartitionSpec as P


HEAD_DIM = 128
CHIPS = 8
CHUNK = 2048
HALF = 1024
SEQ_GROUPS = 2

f32, bf16 = jnp.float32, jnp.bfloat16
BUSY = 1_000_000_000
ANY = pl.BlockSpec(memory_space=pl.ANY)
VMEM = pl.BlockSpec(memory_space=pltpu.VMEM)
SMALL = pltpu.CompilerParams(vmem_limit_bytes=16 << 20)


def near(x):
    return pltpu.with_memory_space_constraint(x, pltpu.VMEM)


def far(x):
    return pltpu.with_memory_space_constraint(x, pltpu.HBM)


def onchip(shape, dtype):
    return pltpu.VMEM(shape, dtype)


def place():
    me = lax.axis_index("tp")
    core = lax.rem(me, 2)
    return me // 2, core, 1 - 2 * core


def chunk_at(chip, steps):
    return lax.rem(chip + steps + 2 * CHIPS, CHIPS)


def columns(start, size):
    return pl.ds(pl.multiple_of(start, HALF), size)


def cost(flops, nbytes):
    return pl.CostEstimate(flops=flops, bytes_accessed=nbytes, transcendentals=0)


def along(x, hops, upward=0, cross=False):
    pairs = []
    for chip in range(CHIPS):
        for core in range(2):
            to = (chip + (hops if core == upward else -hops)) % CHIPS
            pairs.append((2 * chip + core, 2 * to + (1 - core if cross else core)))
    return lax.ppermute(x, "tp", pairs)


def across(x):
    return lax.ppermute(x, "tp", [(i, i ^ 1) for i in range(2 * CHIPS)])


def first_handled(chip, way):
    return [(chunk_at(chip, 3 * way) * CHUNK, CHUNK)]


def handled(chip, core, way):
    return [
        (chunk_at(chip, way) * CHUNK, CHUNK),
        (chunk_at(chip, -2 * way) * CHUNK, CHUNK),
        (chunk_at(chip, 4) * CHUNK + core * HALF, HALF),
        (chip * CHUNK + core * HALF, HALF),
    ]


def fetch(src, dst, ranges, sems):
    copies, at = [], 0
    for start, size in ranges:
        copies.append(
            pltpu.make_async_copy(
                src.at[:, columns(start, size)], dst.at[:, pl.ds(at, size)], sems.at[len(copies)]
            )
        )
        copies[-1].start()
        at += size
    return copies


def first_kernel(p_ref, send_ref, keep_ref, send_sems, keep_sems):
    chip, _, way = place()
    copies = fetch(p_ref, send_ref, first_handled(chip, -way), send_sems)
    copies += fetch(p_ref, keep_ref, first_handled(chip, way), keep_sems)
    for copy in copies:
        copy.wait()


def pack_kernel(p_ref, send_ref, sems):
    chip, core, way = place()
    for copy in fetch(p_ref, send_ref, handled(chip, 1 - core, -way), sems):
        copy.wait()


def first_sum_kernel(keep_ref, got_ref, out_ref):
    out_ref[...] = (keep_ref[...].astype(f32) + got_ref[...].astype(f32)).astype(bf16)


def presum_kernel(p_ref, got_ref, *outs):
    at = 0
    for out, (start, size) in zip(outs, handled(*place())):
        mine = p_ref[:, columns(start, size)].astype(f32)
        out[...] = (mine + got_ref[:, at : at + size].astype(f32)).astype(bf16)
        at += size


def relay_kernel(s2_ref, r3_ref, m_ref):
    m_ref[...] = (s2_ref[...].astype(f32) + r3_ref[...].astype(f32)).astype(bf16)


def arrive_kernel(r1_ref, rm_ref, r4_ref, own_ref, t_ref):
    _, core, _ = place()
    extra = r4_ref[...].astype(f32) + own_ref[...].astype(f32)
    for half in range(2):
        cols = slice(half * HALF, (half + 1) * HALF)
        both = r1_ref[:, cols].astype(f32) + rm_ref[:, cols].astype(f32)
        here = jnp.where(core == half, extra, jnp.zeros_like(extra))
        t_ref[:, cols] = (both + here).astype(bf16)


def hsum_kernel(res_ref, t_ref, rt_ref, n_ref, half_ref):
    chip, core, _ = place()
    total = t_ref[...].astype(f32) + rt_ref[...].astype(f32)
    n = (res_ref[:, columns(chip * CHUNK, CHUNK)].astype(f32) + total).astype(bf16)
    n_ref[...] = n
    half_ref[...] = jnp.where(core == 0, n[:, :HALF], n[:, HALF:])


def pieces(chip, core, way, n, g1, g2, w12, last=None, w34=None):
    opposite = 2 * chunk_at(chip, 4)
    early = [
        (n, 0, 2 * chip, 2),
        (g1, 0, 2 * chunk_at(chip, -way), 2),
        (g2, 0, 2 * chunk_at(chip, -2 * way), 2),
        (w12, 0, 2 * chunk_at(chip, way), 2),
        (w12, CHUNK, 2 * chunk_at(chip, 2 * way), 2),
    ]
    late = [
        (last, 0, 2 * chunk_at(chip, 3 * way), 2),
        (last, CHUNK, opposite + 1 - core, 1),
        (w34, 0, 2 * chunk_at(chip, -3 * way), 2),
        (w34, CHUNK, opposite + core, 1),
    ]
    return early, late


def by_half(wide):
    return [(ref, at + k * HALF, block + k) for ref, at, block, n in wide for k in range(n)]


def write_out(wide, out, sems):
    copies = []
    for i, (ref, at, block, n) in enumerate(wide):
        copies.append(
            pltpu.make_async_copy(
                ref.at[:, pl.ds(at, n * HALF)], out.at[:, columns(block * HALF, n * HALF)], sems.at[i]
            )
        )
        copies[-1].start()
    return copies


def add_squares(wide, sq_ref):
    for ref, at, block in by_half(wide):
        part = jnp.zeros(sq_ref.shape[1:], f32)
        for j in range(0, HALF, 128):
            x = ref[:, at + j : at + j + 128].astype(f32)
            part += x * x
        sq_ref[block] = part


def early_kernel(n_ref, g1_ref, g2_ref, w12_ref, res_out, sq_ref, sems):
    early, _ = pieces(*place(), n_ref, g1_ref, g2_ref, w12_ref)
    copies = write_out(early, res_out, sems)
    sq_ref[...] = jnp.zeros_like(sq_ref)
    add_squares(early, sq_ref)
    for copy in copies:
        copy.wait()


def finish_kernel(
    n_ref, g1_ref, g2_ref, w12_ref, last_ref, w34_ref, gain_ref, early_sq, _,
    res_out, norm_out, peak_out, peak_ref, y_ref, sq_ref, res_sems, norm_sems, peak_sem,
):
    early, late = pieces(*place(), n_ref, g1_ref, g2_ref, w12_ref, last_ref, w34_ref)
    tokens, features = res_out.shape
    copies = write_out(late, res_out, res_sems)
    sq_ref[...] = early_sq[...]
    add_squares(late, sq_ref)
    total = sq_ref[0]
    for block in range(1, features // HALF):
        total += sq_ref[block]
    mean = jnp.sum(total, axis=1, keepdims=True) * (1.0 / features)
    inv = jnp.broadcast_to(lax.rsqrt(mean + 1e-05), (tokens, 128))
    peak = jnp.zeros((tokens, 128), f32)
    for i, (ref, at, block) in enumerate(by_half(early + late)):
        gains = gain_ref[block]
        for j in range(0, HALF, 128):
            x = ref[:, at + j : at + j + 128].astype(f32)
            y = x * inv * gains[:, j : j + 128]
            peak = jnp.maximum(peak, jnp.abs(y))
            y_ref[:, i * HALF + j : i * HALF + j + 128] = y.astype(bf16)
        copies.append(
            pltpu.make_async_copy(
                y_ref.at[:, pl.ds(i * HALF, HALF)],
                norm_out.at[:, columns(block * HALF, HALF)],
                norm_sems.at[i],
            )
        )
        copies[-1].start()
    peak_ref[...] = jnp.max(peak.T, axis=0, keepdims=True)
    copies.append(pltpu.make_async_copy(peak_ref, peak_out, peak_sem))
    copies[-1].start()
    for copy in copies:
        copy.wait()


def attend_kernel(first, q_ref, k_ref, v_ref, len_ref, *refs):
    o_ref, q_rows, o_rows, stage, sem = refs[-5:]
    seqs, width = stage.shape
    heads = width // HEAD_DIM
    rows = seqs * heads
    context = k_ref.shape[1]
    mine = slice(first, first + seqs)
    for h in range(heads):
        cols = slice(h * HEAD_DIM, (h + 1) * HEAD_DIM)
        q_rows[pl.ds(h, seqs, stride=heads), :] = q_ref[mine, cols].astype(f32)
    turned = q_rows[...].T
    owner = lax.broadcasted_iota(jnp.int32, (HEAD_DIM, rows), 1) // heads
    scores = jnp.zeros((context, rows), f32)
    for i in range(seqs):
        own = jnp.where(owner == i, turned, 0.0).astype(bf16)
        scores += jnp.dot(k_ref[first + i], own, preferred_element_type=f32)
    lens = len_ref[mine, :]
    spread = lax.broadcasted_iota(jnp.int32, (seqs, rows), 0)
    spread = spread == lax.broadcasted_iota(jnp.int32, (seqs, rows), 1) // heads
    lens = jnp.sum(jnp.where(spread, lens, 0), axis=0, keepdims=True)
    live = lax.broadcasted_iota(jnp.int32, (context, rows), 0) < lens
    scores = jnp.where(live, scores * (1.0 / math.sqrt(HEAD_DIM)), -1e30)
    expo = jnp.exp(scores - jnp.max(scores, axis=0, keepdims=True))
    probs = (expo * (1.0 / jnp.sum(expo, axis=0, keepdims=True))).T
    for i in range(seqs):
        o_rows[i * heads : (i + 1) * heads, :] = jnp.dot(
            probs[i * heads : (i + 1) * heads, :].astype(bf16),
            v_ref[first + i],
            preferred_element_type=f32,
        )
    for h in range(heads):
        stage[:, h * HEAD_DIM : (h + 1) * HEAD_DIM] = o_rows[
            pl.ds(h, seqs, stride=heads), :
        ].astype(bf16)
    copy = pltpu.make_async_copy(stage, o_ref.at[mine, :], sem)
    copy.start()
    copy.wait()


def attend(queries, keys, values, lens):
    seqs, width = queries.shape
    rows = seqs // SEQ_GROUPS * (width // HEAD_DIM)
    nbytes = 4 * keys.size // SEQ_GROUPS
    out = []
    for g in range(SEQ_GROUPS):
        out = [
            pl.pallas_call(
                functools.partial(attend_kernel, g * (seqs // SEQ_GROUPS)),
                out_shape=jax.ShapeDtypeStruct((seqs, width), bf16),
                in_specs=[VMEM] * 4 + [ANY] * len(out),
                out_specs=ANY,
                scratch_shapes=[
                    pltpu.VMEM((rows, HEAD_DIM), f32),
                    pltpu.VMEM((rows, HEAD_DIM), f32),
                    pltpu.VMEM((seqs // SEQ_GROUPS, width), bf16),
                    pltpu.SemaphoreType.DMA,
                ],
                input_output_aliases={4: 0} if out else {},
                cost_estimate=cost(200_000_000, nbytes),
                compiler_params=SMALL,
            )(queries, keys, values, near(lens), *out)
        ]
    return out[0]


def summed_and_normed(partial, residual, gain):
    tokens, features = partial.shape
    dma = pltpu.SemaphoreType.DMA

    def held(width):
        return onchip((tokens, width), bf16)

    def call(kernel, outs, *args, in_specs=None, loose=0, scratch=(), flops=BUSY):
        args = [far(a) if in_specs else near(a) if i >= loose else a for i, a in enumerate(args)]
        return pl.pallas_call(
            kernel,
            out_shape=outs,
            in_specs=in_specs or [VMEM] * len(args),
            out_specs=jax.tree.map(lambda _: VMEM, outs),
            scratch_shapes=list(scratch),
            cost_estimate=cost(flops, 1 << 20),
            compiler_params=SMALL,
        )(*args)

    send, keep = call(
        first_kernel, (held(CHUNK), held(CHUNK)), partial,
        in_specs=[ANY], scratch=[dma((1,)), dma((1,))], flops=4 * BUSY,
    )
    got = across(send)
    send = call(pack_kernel, held(3 * CHUNK), partial, loose=1, scratch=[dma((4,))], flops=4 * BUSY)
    got_rest = across(send)
    a3 = call(first_sum_kernel, held(CHUNK), keep, got)
    r3 = along(a3, 1, cross=True)
    a1, s2, a4, own = call(
        presum_kernel, (held(CHUNK), held(CHUNK), held(HALF), held(HALF)), partial, got_rest, loose=1
    )
    r1 = along(a1, 1)
    r4 = along(a4, 4)
    m = call(relay_kernel, held(CHUNK), s2, r3)
    rm = along(m, 2, upward=1, cross=True)
    t = call(arrive_kernel, held(CHUNK), r1, rm, r4, own)
    rt = across(t)
    n, half = call(hsum_kernel, (held(CHUNK), held(HALF)), residual, t, rt, loose=1)
    g2 = along(n, 2, upward=1, cross=True)
    g1 = along(n, 1)
    g4 = along(half, 4, cross=True)
    g3 = along(g2, 1, cross=True)
    both = jnp.concatenate([g1, g2], axis=1)
    w12 = across(both)
    last = jnp.concatenate([g3, g4], axis=1)
    w34 = across(last)
    blocks = features // HALF
    gains = gain.astype(f32).reshape(blocks, 1, HALF)
    whole = jax.ShapeDtypeStruct((tokens, features), bf16)
    begun, squares = pl.pallas_call(
        early_kernel,
        out_shape=(whole, onchip((blocks, tokens, 128), f32)),
        in_specs=[VMEM] * 4,
        out_specs=(ANY, VMEM),
        scratch_shapes=[dma((5,))],
        cost_estimate=cost(1_000_000, 1 << 20),
        compiler_params=SMALL,
        name="early",
    )(*map(near, (n, g1, g2, w12)))
    res_out, norm_out, peak = pl.pallas_call(
        finish_kernel,
        out_shape=(whole, whole, jax.ShapeDtypeStruct((1, tokens), f32)),
        in_specs=[VMEM] * 8 + [ANY],
        out_specs=(ANY, ANY, ANY),
        scratch_shapes=[
            pltpu.VMEM((1, tokens), f32),
            pltpu.VMEM((tokens, features), bf16),
            pltpu.VMEM((blocks, tokens, 128), f32),
            dma((4,)),
            dma((blocks,)),
            dma,
        ],
        input_output_aliases={8: 0},
        cost_estimate=cost(1_000_000, 4 << 20),
        compiler_params=SMALL,
        name="finish",
    )(*map(near, (n, g1, g2, w12, last, w34, gains, squares)), begun)
    return res_out, norm_out, peak.reshape(tokens)


def on_device(partials, residual, gain, queries, key_cache, value_cache, lengths):
    lens = jnp.broadcast_to(lengths[:, None], (lengths.shape[0], 128))
    attended = attend(queries, key_cache[0], value_cache[0], lens)
    new_residual, normed, token_peak = summed_and_normed(partials[0], residual, gain)
    return (new_residual, normed, token_peak, attended)


def solution(mesh):
    return jax.shard_map(
        on_device,
        mesh=mesh,
        in_specs=(
            P("tp", "dp", None),
            P("dp", None),
            P(),
            P("dp", "tp"),
            P("tp", "dp", None, None),
            P("tp", "dp", None, None),
            P("dp"),
        ),
        out_specs=(P("dp", None), P("dp", None), P("dp"), P("dp", "tp")),
        check_vma=False,
    )
```

```python
import functools
import math

import jax
import jax.numpy as jnp
from jax import lax
from jax.experimental import pallas as pl
from jax.experimental.pallas import tpu as pltpu
from jax.sharding import PartitionSpec as P


HEAD_DIM = 128
CHIPS = 8
CHUNK = 2048
HALF = 1024
SEQ_GROUPS = 2

f32, bf16 = jnp.float32, jnp.bfloat16
BUSY = 1_000_000_000
ANY = pl.BlockSpec(memory_space=pl.ANY)
VMEM = pl.BlockSpec(memory_space=pltpu.VMEM)
SMALL = pltpu.CompilerParams(vmem_limit_bytes=16 << 20)


def near(x):
    return pltpu.with_memory_space_constraint(x, pltpu.VMEM)


def far(x):
    return pltpu.with_memory_space_constraint(x, pltpu.HBM)


def onchip(shape, dtype):
    return pltpu.VMEM(shape, dtype)


def place():
    me = lax.axis_index("tp")
    core = lax.rem(me, 2)
    return me // 2, core, 1 - 2 * core


def chunk_at(chip, steps):
    return lax.rem(chip + steps + 2 * CHIPS, CHIPS)


def columns(start, size):
    return pl.ds(pl.multiple_of(start, HALF), size)


def cost(flops, nbytes):
    return pl.CostEstimate(flops=flops, bytes_accessed=nbytes, transcendentals=0)


def along(x, hops, upward=0, cross=False):
    pairs = []
    for chip in range(CHIPS):
        for core in range(2):
            to = (chip + (hops if core == upward else -hops)) % CHIPS
            pairs.append((2 * chip + core, 2 * to + (1 - core if cross else core)))
    return lax.ppermute(x, "tp", pairs)


def across(x):
    return lax.ppermute(x, "tp", [(i, i ^ 1) for i in range(2 * CHIPS)])


def first_handled(chip, way):
    return [(chunk_at(chip, 3 * way) * CHUNK, CHUNK)]


def handled(chip, core, way):
    return [
        (chunk_at(chip, way) * CHUNK, CHUNK),
        (chunk_at(chip, -2 * way) * CHUNK, CHUNK),
        (chunk_at(chip, 4) * CHUNK + core * HALF, HALF),
        (chip * CHUNK + core * HALF, HALF),
    ]


def fetch(src, dst, ranges, sems):
    copies, at = [], 0
    for start, size in ranges:
        copies.append(
            pltpu.make_async_copy(
                src.at[:, columns(start, size)], dst.at[:, pl.ds(at, size)], sems.at[len(copies)]
            )
        )
        copies[-1].start()
        at += size
    return copies


def first_kernel(p_ref, send_ref, keep_ref, send_sems, keep_sems):
    chip, _, way = place()
    copies = fetch(p_ref, send_ref, first_handled(chip, -way), send_sems)
    copies += fetch(p_ref, keep_ref, first_handled(chip, way), keep_sems)
    for copy in copies:
        copy.wait()


def pack_kernel(p_ref, send_ref, sems):
    chip, core, way = place()
    for copy in fetch(p_ref, send_ref, handled(chip, 1 - core, -way), sems):
        copy.wait()


def first_sum_kernel(keep_ref, got_ref, out_ref):
    out_ref[...] = (keep_ref[...].astype(f32) + got_ref[...].astype(f32)).astype(bf16)


def presum_kernel(p_ref, got_ref, *outs):
    at = 0
    for out, (start, size) in zip(outs, handled(*place())):
        mine = p_ref[:, columns(start, size)].astype(f32)
        out[...] = (mine + got_ref[:, at : at + size].astype(f32)).astype(bf16)
        at += size


def relay_kernel(s2_ref, r3_ref, m_ref):
    m_ref[...] = (s2_ref[...].astype(f32) + r3_ref[...].astype(f32)).astype(bf16)


def arrive_kernel(r1_ref, rm_ref, r4_ref, own_ref, t_ref):
    _, core, _ = place()
    extra = r4_ref[...].astype(f32) + own_ref[...].astype(f32)
    for half in range(2):
        cols = slice(half * HALF, (half + 1) * HALF)
        both = r1_ref[:, cols].astype(f32) + rm_ref[:, cols].astype(f32)
        here = jnp.where(core == half, extra, jnp.zeros_like(extra))
        t_ref[:, cols] = (both + here).astype(bf16)


def hsum_kernel(res_ref, t_ref, rt_ref, n_ref, half_ref):
    chip, core, _ = place()
    total = t_ref[...].astype(f32) + rt_ref[...].astype(f32)
    n = (res_ref[:, columns(chip * CHUNK, CHUNK)].astype(f32) + total).astype(bf16)
    n_ref[...] = n
    half_ref[...] = jnp.where(core == 0, n[:, :HALF], n[:, HALF:])


def pieces(chip, core, way, n, g1, g2, w12, last=None, w34=None):
    opposite = 2 * chunk_at(chip, 4)
    early = [
        (n, 0, 2 * chip, 2),
        (g1, 0, 2 * chunk_at(chip, -way), 2),
        (g2, 0, 2 * chunk_at(chip, -2 * way), 2),
        (w12, 0, 2 * chunk_at(chip, way), 2),
        (w12, CHUNK, 2 * chunk_at(chip, 2 * way), 2),
    ]
    late = [
        (last, 0, 2 * chunk_at(chip, 3 * way), 2),
        (last, CHUNK, opposite + 1 - core, 1),
        (w34, 0, 2 * chunk_at(chip, -3 * way), 2),
        (w34, CHUNK, opposite + core, 1),
    ]
    return early, late


def by_half(wide):
    return [(ref, at + k * HALF, block + k) for ref, at, block, n in wide for k in range(n)]


def write_out(wide, out, sems):
    copies = []
    for i, (ref, at, block, n) in enumerate(wide):
        copies.append(
            pltpu.make_async_copy(
                ref.at[:, pl.ds(at, n * HALF)], out.at[:, columns(block * HALF, n * HALF)], sems.at[i]
            )
        )
        copies[-1].start()
    return copies


def add_squares(wide, sq_ref):
    for ref, at, block in by_half(wide):
        part = jnp.zeros(sq_ref.shape[1:], f32)
        for j in range(0, HALF, 128):
            x = ref[:, at + j : at + j + 128].astype(f32)
            part += x * x
        sq_ref[block] = part


def early_kernel(n_ref, g1_ref, g2_ref, w12_ref, gain_ref, res_out, sq_ref, gained_ref, top_ref, sems):
    early, _ = pieces(*place(), n_ref, g1_ref, g2_ref, w12_ref)
    copies = write_out(early, res_out, sems)
    sq_ref[...] = jnp.zeros_like(sq_ref)
    add_squares(early, sq_ref)
    top = jnp.zeros(top_ref.shape, f32)
    for i, (ref, at, block) in enumerate(by_half(early)):
        gains = gain_ref[block]
        for j in range(0, HALF, 128):
            x = ref[:, at + j : at + j + 128].astype(f32) * gains[:, j : j + 128]
            top = jnp.maximum(top, jnp.abs(x))
            gained_ref[:, i * HALF + j : i * HALF + j + 128] = x
    top_ref[...] = top
    for copy in copies:
        copy.wait()


def finish_kernel(
    n_ref, g1_ref, g2_ref, w12_ref, last_ref, w34_ref, gain_ref, early_sq, gained_ref, top_ref, _,
    res_out, norm_out, peak_out, peak_ref, y_ref, sq_ref, res_sems, norm_sems, peak_sem,
):
    early, late = pieces(*place(), n_ref, g1_ref, g2_ref, w12_ref, last_ref, w34_ref)
    tokens, features = res_out.shape
    copies = write_out(late, res_out, res_sems)
    sq_ref[...] = early_sq[...]
    add_squares(late, sq_ref)
    total = sq_ref[0]
    for block in range(1, features // HALF):
        total += sq_ref[block]
    mean = jnp.sum(total, axis=1, keepdims=True) * (1.0 / features)
    inv = jnp.broadcast_to(lax.rsqrt(mean + 1e-05), (tokens, 128))
    peak = top_ref[...] * inv
    ready = len(by_half(early))
    for i, (ref, at, block) in enumerate(by_half(early + late)):
        gains = gain_ref[block]
        for j in range(0, HALF, 128):
            if i < ready:
                y = gained_ref[:, i * HALF + j : i * HALF + j + 128] * inv
            else:
                x = ref[:, at + j : at + j + 128].astype(f32)
                y = x * gains[:, j : j + 128] * inv
                peak = jnp.maximum(peak, jnp.abs(y))
            y_ref[:, i * HALF + j : i * HALF + j + 128] = y.astype(bf16)
        copies.append(
            pltpu.make_async_copy(
                y_ref.at[:, pl.ds(i * HALF, HALF)],
                norm_out.at[:, columns(block * HALF, HALF)],
                norm_sems.at[i],
            )
        )
        copies[-1].start()
    peak_ref[...] = jnp.max(peak.T, axis=0, keepdims=True)
    copies.append(pltpu.make_async_copy(peak_ref, peak_out, peak_sem))
    copies[-1].start()
    for copy in copies:
        copy.wait()


def attend_kernel(first, q_ref, k_ref, v_ref, len_ref, *refs):
    o_ref, q_rows, o_rows, stage, sem = refs[-5:]
    seqs, width = stage.shape
    heads = width // HEAD_DIM
    rows = seqs * heads
    context = k_ref.shape[1]
    mine = slice(first, first + seqs)
    for h in range(heads):
        cols = slice(h * HEAD_DIM, (h + 1) * HEAD_DIM)
        q_rows[pl.ds(h, seqs, stride=heads), :] = q_ref[mine, cols].astype(f32)
    turned = q_rows[...].T
    owner = lax.broadcasted_iota(jnp.int32, (HEAD_DIM, rows), 1) // heads
    scores = jnp.zeros((context, rows), f32)
    for i in range(seqs):
        own = jnp.where(owner == i, turned, 0.0).astype(bf16)
        scores += jnp.dot(k_ref[first + i], own, preferred_element_type=f32)
    lens = len_ref[mine, :]
    spread = lax.broadcasted_iota(jnp.int32, (seqs, rows), 0)
    spread = spread == lax.broadcasted_iota(jnp.int32, (seqs, rows), 1) // heads
    lens = jnp.sum(jnp.where(spread, lens, 0), axis=0, keepdims=True)
    live = lax.broadcasted_iota(jnp.int32, (context, rows), 0) < lens
    scores = jnp.where(live, scores * (1.0 / math.sqrt(HEAD_DIM)), -1e30)
    expo = jnp.exp(scores - jnp.max(scores, axis=0, keepdims=True))
    probs = (expo * (1.0 / jnp.sum(expo, axis=0, keepdims=True))).T
    for i in range(seqs):
        o_rows[i * heads : (i + 1) * heads, :] = jnp.dot(
            probs[i * heads : (i + 1) * heads, :].astype(bf16),
            v_ref[first + i],
            preferred_element_type=f32,
        )
    for h in range(heads):
        stage[:, h * HEAD_DIM : (h + 1) * HEAD_DIM] = o_rows[
            pl.ds(h, seqs, stride=heads), :
        ].astype(bf16)
    copy = pltpu.make_async_copy(stage, o_ref.at[mine, :], sem)
    copy.start()
    copy.wait()


def attend(queries, keys, values, lens):
    seqs, width = queries.shape
    rows = seqs // SEQ_GROUPS * (width // HEAD_DIM)
    nbytes = 4 * keys.size // SEQ_GROUPS
    out = []
    for g in range(SEQ_GROUPS):
        out = [
            pl.pallas_call(
                functools.partial(attend_kernel, g * (seqs // SEQ_GROUPS)),
                out_shape=jax.ShapeDtypeStruct((seqs, width), bf16),
                in_specs=[VMEM] * 4 + [ANY] * len(out),
                out_specs=ANY,
                scratch_shapes=[
                    pltpu.VMEM((rows, HEAD_DIM), f32),
                    pltpu.VMEM((rows, HEAD_DIM), f32),
                    pltpu.VMEM((seqs // SEQ_GROUPS, width), bf16),
                    pltpu.SemaphoreType.DMA,
                ],
                input_output_aliases={4: 0} if out else {},
                cost_estimate=cost(200_000_000, nbytes),
                compiler_params=SMALL,
            )(queries, keys, values, near(lens), *out)
        ]
    return out[0]


def summed_and_normed(partial, residual, gain):
    tokens, features = partial.shape
    dma = pltpu.SemaphoreType.DMA

    def held(width):
        return onchip((tokens, width), bf16)

    def call(kernel, outs, *args, in_specs=None, loose=0, scratch=(), flops=BUSY):
        args = [far(a) if in_specs else near(a) if i >= loose else a for i, a in enumerate(args)]
        return pl.pallas_call(
            kernel,
            out_shape=outs,
            in_specs=in_specs or [VMEM] * len(args),
            out_specs=jax.tree.map(lambda _: VMEM, outs),
            scratch_shapes=list(scratch),
            cost_estimate=cost(flops, 1 << 20),
            compiler_params=SMALL,
        )(*args)

    send, keep = call(
        first_kernel, (held(CHUNK), held(CHUNK)), partial,
        in_specs=[ANY], scratch=[dma((1,)), dma((1,))], flops=4 * BUSY,
    )
    got = across(send)
    send = call(pack_kernel, held(3 * CHUNK), partial, loose=1, scratch=[dma((4,))], flops=4 * BUSY)
    got_rest = across(send)
    a3 = call(first_sum_kernel, held(CHUNK), keep, got)
    r3 = along(a3, 1, cross=True)
    a1, s2, a4, own = call(
        presum_kernel, (held(CHUNK), held(CHUNK), held(HALF), held(HALF)), partial, got_rest, loose=1
    )
    r1 = along(a1, 1)
    r4 = along(a4, 4)
    m = call(relay_kernel, held(CHUNK), s2, r3)
    rm = along(m, 2, upward=1, cross=True)
    t = call(arrive_kernel, held(CHUNK), r1, rm, r4, own)
    rt = across(t)
    n, half = call(hsum_kernel, (held(CHUNK), held(HALF)), residual, t, rt, loose=1)
    g2 = along(n, 2, upward=1, cross=True)
    g1 = along(n, 1)
    g4 = along(half, 4, cross=True)
    g3 = along(g2, 1, cross=True)
    both = jnp.concatenate([g1, g2], axis=1)
    w12 = across(both)
    last = jnp.concatenate([g3, g4], axis=1)
    w34 = across(last)
    blocks = features // HALF
    gains = gain.astype(f32).reshape(blocks, 1, HALF)
    whole = jax.ShapeDtypeStruct((tokens, features), bf16)
    begun, squares, gained, top = pl.pallas_call(
        early_kernel,
        out_shape=(
            whole,
            onchip((blocks, tokens, 128), f32),
            onchip((tokens, 5 * CHUNK), f32),
            onchip((tokens, 128), f32),
        ),
        in_specs=[VMEM] * 5,
        out_specs=(ANY, VMEM, VMEM, VMEM),
        scratch_shapes=[dma((5,))],
        cost_estimate=cost(1_000_000, 1 << 20),
        compiler_params=SMALL,
        name="early",
    )(*map(near, (n, g1, g2, w12, gains)))
    res_out, norm_out, peak = pl.pallas_call(
        finish_kernel,
        out_shape=(whole, whole, jax.ShapeDtypeStruct((1, tokens), f32)),
        in_specs=[VMEM] * 10 + [ANY],
        out_specs=(ANY, ANY, ANY),
        scratch_shapes=[
            pltpu.VMEM((1, tokens), f32),
            pltpu.VMEM((tokens, features), bf16),
            pltpu.VMEM((blocks, tokens, 128), f32),
            dma((4,)),
            dma((blocks,)),
            dma,
        ],
        input_output_aliases={10: 0},
        cost_estimate=cost(1_000_000, 4 << 20),
        compiler_params=SMALL,
        name="finish",
    )(*map(near, (n, g1, g2, w12, last, w34, gains, squares, gained, top)), begun)
    return res_out, norm_out, peak.reshape(tokens)


def on_device(partials, residual, gain, queries, key_cache, value_cache, lengths):
    lens = jnp.broadcast_to(lengths[:, None], (lengths.shape[0], 128))
    attended = attend(queries, key_cache[0], value_cache[0], lens)
    new_residual, normed, token_peak = summed_and_normed(partials[0], residual, gain)
    return (new_residual, normed, token_peak, attended)


def solution(mesh):
    return jax.shard_map(
        on_device,
        mesh=mesh,
        in_specs=(
            P("tp", "dp", None),
            P("dp", None),
            P(),
            P("dp", "tp"),
            P("tp", "dp", None, None),
            P("tp", "dp", None, None),
            P("dp"),
        ),
        out_specs=(P("dp", None), P("dp", None), P("dp"), P("dp", "tp")),
        check_vma=False,
    )
```
